32 devices in a mesh: tm: 4 (over y, x), sky: 8 (over z, core).
Axes of the slice: x: 2, y: 2, z: 4, core: 2. Of those that a mesh axis runs over, the one named last changes fastest.
Arguments:
- residual: float32 [16384, 128], P(('tm', 'sky')), may hold values from -110 to 110
- obs_weight: float32 [16384, 128], P(('tm', 'sky')), may hold values from 0.5 to 2
- source_partials: float32 [5, 16384, 128], P(None, ('tm', 'sky')), may hold values from -1 to 1
- attitude_partials: float32 [16, 16384, 128], P(None, ('tm', 'sky')), may hold values from -1.5 to 1.5
- source_index: int32 [16384, 128], P(('tm', 'sky')), may hold values from 0 to 127
- tile_pixel: int32 [16384], P(('tm', 'sky')), may hold values from 0 to 1023, as said below
- tile_knot: int32 [16384], P(('tm', 'sky')), may hold values from 0 to 2047, as said below
- pixel_slot: int32 [1024], replicated, may hold values from 0 to 1023, as said below
Outputs:
- final_residual: float32 [16384, 128], P(('tm', 'sky'))
- source_update: float32 [5, 131072], P(None, 'sky')
- attitude_update: float32 [4, 2048], P(None, 'tm')
The draws below stay inside these ranges and needn't reach their ends.
Inputs may be any that keep to these rules, and one draw needn't show every extreme that they name: Tiles come in aligned blocks of 512; with owner = pixel_slot[tile_pixel[t]] // 128, no block holds more than 192 tiles of one owner, and every block holds exactly 192 tiles of some owner. `pixel_slot`: every slot number appears once. `tile_knot`: the tiles of aligned block q of 512 tiles have first knots in [q * 64, (q + 1) * 64).
All inputs are finite; a program needn't handle non-finite values.
Results may differ from the reference program's by a relative error of at most 0.0003.
Values sent between devices are 32-bit elements; how exact they have to be, the bound alone decides.
A program may use at most 128 MiB of HBM per device.

```python
import math
import jax
import jax.numpy as jnp
from jax import lax

OBS_TILE = 128
TILES_DEV = 512
PIX_DEV = 128
SRC_PIX = 128
OWNERS = 8
TIME_SHARDS = 4
CAP = 192
SPAN = 64
PIXELS = 1024
KNOTS = 2048
TILES = 16384


def sky_layout(key):
    slot_of_pixel = jax.random.permutation(jax.random.fold_in(key, 11), PIXELS).astype(jnp.int32)
    pixel_of_slot = jnp.argsort(slot_of_pixel, stable=True).astype(jnp.int32)
    blocks = TILES // TILES_DEV
    crowded_rows = jax.random.randint(jax.random.fold_in(key, 12), (TIME_SHARDS,), 0, OWNERS)
    crowded = crowded_rows[jnp.arange(blocks, dtype=jnp.int32) // OWNERS]
    positions = jnp.arange(TILES_DEV, dtype=jnp.int32)
    remaining = positions - CAP
    plain_owner = (crowded[:, None] + 1 + remaining[None, :] % (OWNERS - 1)) % OWNERS
    owner_ids = jnp.where(positions[None, :] < CAP, crowded[:, None], plain_owner)
    shuffles = jax.vmap(lambda sub: jax.random.permutation(sub, TILES_DEV))(jax.random.split(jax.random.fold_in(key, 13), blocks))
    owner_ids = jnp.take_along_axis(owner_ids, shuffles, axis=1)
    local_pixel = jax.random.randint(jax.random.fold_in(key, 14), (blocks, TILES_DEV), 0, PIX_DEV)
    pixel_ids = pixel_of_slot[(owner_ids * PIX_DEV + local_pixel).reshape(-1)]
    return (slot_of_pixel, pixel_ids.astype(jnp.int32))


def draw_pixel_slot(key, part):
    return sky_layout(key)[0]


def draw_tile_pixel(key, part):
    return sky_layout(key)[1]


def knot_starts(key):
    offset = jax.random.randint(jax.random.fold_in(key, 21), (TILES,), 0, SPAN)
    return (jnp.arange(TILES, dtype=jnp.int32) // TILES_DEV * SPAN + offset).astype(jnp.int32)


def draw_tile_knot(key, part):
    return knot_starts(key)


def attitude_parts(key):
    partials = jnp.clip(0.25 * jax.random.normal(jax.random.fold_in(key, 31), (16, TILES, OBS_TILE), jnp.float32), -1.5, 1.5)
    return partials


def draw_attitude_partials(key, part):
    return attitude_parts(key)


def draw_residual(key, part):
    partials = attitude_parts(key)
    knot_start = knot_starts(key)
    attitude_curve = jnp.clip(jax.random.normal(jax.random.fold_in(key, 32), (4, KNOTS + 3), jnp.float32), -4.0, 4.0)
    signal = jnp.clip(jax.random.normal(jax.random.fold_in(key, 33), (TILES, OBS_TILE), jnp.float32), -6.0, 6.0)
    for segment in range(4):
        values = jnp.take(attitude_curve, knot_start + segment, axis=1)
        for component in range(4):
            signal = signal + partials[4 * segment + component] * values[component][:, None]
    return signal


def with_ends(values, rng, low, high):
    shape = values.shape
    spot = [jax.random.randint(jax.random.fold_in(rng, axis), (), 0, shape[axis]) for axis in range(len(shape))]
    values = values.at[tuple(spot)].set(low)
    longest = shape.index(max(shape))
    spot[longest] = (spot[longest] + 1) % shape[longest]
    return values.at[tuple(spot)].set(high)


def shard_levels(key, extent, cuts, low, top_value):
    gain, own = 1.0, jax.random.fold_in(key, 6)
    for axis_at, blocks in cuts:
        heights = jnp.exp(jax.random.uniform(jax.random.fold_in(own, axis_at), (blocks,), jnp.float32, low / len(cuts), top_value / len(cuts)))
        gain = gain * jnp.repeat(heights, extent[axis_at] // blocks).reshape([-1 if axis == axis_at else 1 for axis in range(len(extent))])
    return gain


def centred(own_key, extent, width, reach, cuts=(), kind=jnp.bfloat16):
    values = width * jax.random.normal(own_key, extent, jnp.float32)
    if cuts:
        values = values * shard_levels(own_key, extent, cuts, -0.22, 0.18)
    return jnp.clip(values, -reach, reach).astype(kind)


def setup_inputs(seed: int = 0) -> dict:
    arg_keys = jax.random.split(jax.random.key(seed), 9)
    return {
        "residual": draw_residual(jax.random.fold_in(arg_keys[8], 71), 0),
        "obs_weight": jnp.clip(jnp.exp(math.log(2.0) - 1.3862944 * jax.random.uniform(arg_keys[1], (TILES, OBS_TILE), jnp.float32) ** shard_levels(arg_keys[1], (TILES, OBS_TILE), ((0, 32),), -0.2, 0.2)), 0.5, 2.0),
        "source_partials": centred(arg_keys[2], (5, TILES, OBS_TILE), 32 ** -0.5, 1.0, ((1, 32),), jnp.float32),
        "attitude_partials": draw_attitude_partials(jax.random.fold_in(arg_keys[8], 71), 0),
        "source_index": with_ends(jax.random.randint(arg_keys[4], (TILES, OBS_TILE), 0, SRC_PIX), jax.random.fold_in(arg_keys[4], 1), 0, SRC_PIX - 1).astype(jnp.int32),
        "tile_pixel": draw_tile_pixel(jax.random.fold_in(arg_keys[8], 71), 0),
        "tile_knot": draw_tile_knot(jax.random.fold_in(arg_keys[8], 71), 0),
        "pixel_slot": draw_pixel_slot(jax.random.fold_in(arg_keys[8], 71), 0),
    }


SOURCE_PAIRS = tuple(((first, second) for first in range(5) for second in range(first, 5)))
KNOT_PAIRS = tuple(((first, second) for first in range(4) for second in range(first, 4)))

def damped_solve(normal, target, order, pairs):
    entries = {}
    for number, couple in enumerate(pairs):
        entries[couple] = normal[number]
    factor = {}
    for column in range(order):
        pivot_value = entries[column, column] + 1.0
        for earlier in range(column):
            pivot_value = pivot_value - factor[column, earlier] * factor[column, earlier]
        pivot_value = jnp.sqrt(pivot_value)
        factor[column, column] = pivot_value
        for below in range(column + 1, order):
            current = entries[column, below]
            for earlier in range(column):
                current = current - factor[below, earlier] * factor[column, earlier]
            factor[below, column] = current / pivot_value
    forward = []
    for column in range(order):
        current = target[column]
        for earlier in range(column):
            current = current - factor[column, earlier] * forward[earlier]
        forward.append(current / factor[column, column])
    answer = [None] * order
    for column in reversed(range(order)):
        current = forward[column]
        for later in range(column + 1, order):
            current = current - factor[later, column] * answer[later]
        answer[column] = current / factor[column, column]
    return jnp.stack(answer)

def source_terms(weights, partials, baseline):
    products = [weights * partials[first] * partials[second] for first, second in SOURCE_PAIRS]
    products = products + [weights * partials[first] * baseline for first in range(5)]
    return products

def knot_terms(weights, partials, baseline):
    result = []
    for segment in range(4):
        portion = partials[4 * segment:4 * segment + 4]
        sums_rows = [lax.optimization_barrier(jnp.sum(weights * portion[first] * portion[second], axis=-1)) for first, second in KNOT_PAIRS]
        sums_rows = sums_rows + [lax.optimization_barrier(jnp.sum(weights * portion[first] * baseline, axis=-1)) for first in range(4)]
        result.append(jnp.stack(sums_rows))
    return result

def correct(baseline, partials, picked):
    accumulated = partials[0] * picked[0]
    for component in range(1, partials.shape[0]):
        accumulated = accumulated + partials[component] * picked[component]
    return baseline - accumulated

def knot_correct(baseline, partials, extended, knot_start):
    accumulated = None
    for segment in range(4):
        values = jnp.take(extended, knot_start + segment, axis=1)
        for component in range(4):
            addend = partials[4 * segment + component] * values[component][:, None]
            accumulated = addend if accumulated is None else accumulated + addend
    return baseline - accumulated

def reference(residual, obs_weight, source_partials, attitude_partials, source_index, tile_pixel, tile_knot, pixel_slot):
    blocks = residual.shape[0] // TILES_DEV
    sources = pixel_slot.shape[0] * SRC_PIX
    source_id = (jnp.take(pixel_slot, tile_pixel)[:, None] * SRC_PIX + source_index).astype(jnp.int32)

    def add_block(running, number):
        offset = (number * TILES_DEV).astype(jnp.int32)
        baseline = lax.dynamic_slice_in_dim(residual, offset, TILES_DEV, 0)
        weights = lax.dynamic_slice_in_dim(obs_weight, offset, TILES_DEV, 0)
        partials = lax.dynamic_slice_in_dim(source_partials, offset, TILES_DEV, 1)
        indices = lax.dynamic_slice_in_dim(source_id, offset, TILES_DEV, 0)
        stacked = jnp.stack(source_terms(weights, partials, baseline), axis=-1).reshape(-1, 20)
        return (running + jax.ops.segment_sum(stacked, indices.reshape(-1), num_segments=sources), None)
    normals, _ = lax.scan(add_block, jnp.zeros((sources, 20), jnp.float32), jnp.arange(blocks, dtype=jnp.int32))
    normals = normals.T
    source_update = damped_solve(normals[:15], normals[15:], 5, SOURCE_PAIRS)
    picked = jnp.take(source_update, source_id, axis=1)
    settled = correct(residual, source_partials, picked)
    knots = KNOTS
    accumulated = jnp.zeros((14, knots + 3), jnp.float32)
    for segment, tile_sums in enumerate(knot_terms(obs_weight, attitude_partials, settled)):
        accumulated = accumulated + jax.ops.segment_sum(tile_sums.T, tile_knot + segment, num_segments=knots + 3).T
    attitude_update = damped_solve(accumulated[:10, :knots], accumulated[10:, :knots], 4, KNOT_PAIRS)
    extended = jnp.concatenate([attitude_update, jnp.zeros((4, 3), jnp.float32)], axis=1)
    final_residual = knot_correct(settled, attitude_partials, extended, tile_knot)
    return (final_residual, source_update, attitude_update)
```

```python
import functools

import jax
import jax.numpy as jnp
from jax import lax
from jax.experimental import pallas as pl
from jax.experimental.pallas import tpu as pltpu
from jax.sharding import PartitionSpec as P

PIX_DEV = 128
SRC_PIX = 128
KNOTS_DEV = 512


SOURCE_PAIRS = tuple(((first, second) for first in range(5) for second in range(first, 5)))
KNOT_PAIRS = tuple(((first, second) for first in range(4) for second in range(first, 4)))


def passed_along(value, axes, steps):
    count = 1
    for axis in axes:
        count *= lax.axis_size(axis)
    first, last = (max(0, -steps), min(count, count - steps))
    return lax.ppermute(value, axes, [(source, source + steps) for source in range(first, last)])


def damped_solve(normal, target, order, pairs):
    entries = {}
    for number, couple in enumerate(pairs):
        entries[couple] = normal[number]
    factor = {}
    for column in range(order):
        pivot_value = entries[column, column] + 1.0
        for earlier in range(column):
            pivot_value = pivot_value - factor[column, earlier] * factor[column, earlier]
        pivot_value = jnp.sqrt(pivot_value)
        factor[column, column] = pivot_value
        for below in range(column + 1, order):
            current = entries[column, below]
            for earlier in range(column):
                current = current - factor[below, earlier] * factor[column, earlier]
            factor[below, column] = current / pivot_value
    forward = []
    for column in range(order):
        current = target[column]
        for earlier in range(column):
            current = current - factor[column, earlier] * forward[earlier]
        forward.append(current / factor[column, column])
    answer = [None] * order
    for column in reversed(range(order)):
        current = forward[column]
        for later in range(column + 1, order):
            current = current - factor[later, column] * answer[later]
        answer[column] = current / factor[column, column]
    return jnp.stack(answer)


ROWS = 20
PAD = 24


def sums_kernel(pixel_ref, slot_ref, resid, weight, parts, index, out, acc, stage):
    tiles = resid.shape[0]
    chunks, _, run, _ = out.shape
    pixels = chunks * run

    def clear(step, carry):
        acc[pl.ds(pl.multiple_of(step * 192, 192), 192), :] = jnp.zeros((192, SRC_PIX), jnp.float32)
        return carry

    lax.fori_loop(0, pixels * PAD // 192, clear, 0)
    stage[...] = jnp.zeros_like(stage)
    sources = lax.broadcasted_iota(jnp.int32, (SRC_PIX, SRC_PIX), 0)

    def group(step, carry):
        base = pl.multiple_of(step * 8, 8)
        here = pl.ds(base, 8)
        fields = [parts[c, here, :] for c in range(5)]
        scaled = [weight[here, :] * field for field in fields]
        baseline = resid[here, :]
        row = 0
        for first, second in SOURCE_PAIRS:
            stage[pl.ds(row, 8, stride=PAD), :] = scaled[first] * fields[second]
            row += 1
        for first in range(5):
            stage[pl.ds(row, 8, stride=PAD), :] = scaled[first] * baseline
            row += 1
        ids = index[here, :]
        for j in range(8):
            seat = slot_ref[pixel_ref[base + j]]
            values = stage[j * PAD : (j + 1) * PAD, :]
            high = values.astype(jnp.bfloat16)
            low = (values - high.astype(jnp.float32)).astype(jnp.bfloat16)
            hits = jnp.where(sources == ids[j : j + 1, :], 1.0, 0.0).astype(jnp.bfloat16)
            both = lax.dot_general(
                jnp.concatenate([high, low], axis=0),
                hits,
                (((1,), (1,)), ((), ())),
                preferred_element_type=jnp.float32,
            )
            spot = pl.ds(pl.multiple_of(seat * PAD, 8), PAD)
            acc[spot, :] += both[:PAD] + both[PAD:]
        return carry

    lax.fori_loop(0, tiles // 8, group, 0)

    def unload(chunk, carry):
        for row in range(ROWS):
            for part in range(run // 8):
                start = (chunk * run + part * 8) * PAD + row
                out[chunk, row, part * 8 : part * 8 + 8, :] = acc[pl.ds(start, 8, stride=PAD), :]
        return carry

    lax.fori_loop(0, chunks, unload, 0)


def local_sums(tile_pixel, pixel_slot, residual, obs_weight, source_partials, source_index, chunks):
    pixels = pixel_slot.shape[0]
    return pl.pallas_call(
        sums_kernel,
        name="local_sums",
        out_shape=jax.ShapeDtypeStruct((chunks, ROWS, pixels // chunks, SRC_PIX), jnp.float32),
        in_specs=[pl.BlockSpec(memory_space=pltpu.SMEM)] * 2
        + [pl.BlockSpec(memory_space=pltpu.VMEM)] * 4,
        out_specs=pl.BlockSpec(memory_space=pltpu.VMEM),
        scratch_shapes=[
            pltpu.VMEM((pixels * PAD, SRC_PIX), jnp.float32),
            pltpu.VMEM((8 * PAD, SRC_PIX), jnp.float32),
        ],
        compiler_params=pltpu.CompilerParams(vmem_limit_bytes=60 * 1024 * 1024),
    )(tile_pixel, pixel_slot, residual, obs_weight, source_partials, source_index)


def settle_kernel(run, pixel_ref, slot_ref, resid, parts, index, table, out, rows):
    tiles = resid.shape[0]

    def group(step, carry):
        base = pl.multiple_of(step * 8, 8)
        here = pl.ds(base, 8)
        for j in range(8):
            seat = slot_ref[pixel_ref[base + j]]
            start = (seat // run) * (5 * run) + seat % run
            for c in range(5):
                rows[c, pl.ds(base + j, 1), :] = table[pl.ds(start + c * run, 1), :]
        ids = index[here, :]
        total = None
        for c in range(5):
            picked = jnp.take_along_axis(rows[c, here, :], ids, axis=1)
            addend = parts[c, here, :] * picked
            total = addend if total is None else total + addend
        out[here, :] = resid[here, :] - total
        return carry

    lax.fori_loop(0, tiles // 8, group, 0)


def settle(tile_pixel, pixel_slot, residual, source_partials, source_index, table, run):
    tiles = residual.shape[0]
    return pl.pallas_call(
        functools.partial(settle_kernel, run),
        name="settle",
        out_shape=jax.ShapeDtypeStruct(residual.shape, jnp.float32),
        in_specs=[pl.BlockSpec(memory_space=pltpu.SMEM)] * 2
        + [pl.BlockSpec(memory_space=pltpu.VMEM)] * 4,
        out_specs=pl.BlockSpec(memory_space=pltpu.VMEM),
        scratch_shapes=[pltpu.VMEM((5, tiles, SRC_PIX), jnp.float32)],
        compiler_params=pltpu.CompilerParams(vmem_limit_bytes=48 * 1024 * 1024),
    )(tile_pixel, pixel_slot, residual, source_partials, source_index, table)


def tile_rows(weights, partials, baseline, couples):
    rows = []
    for segment in range(4):
        portion = partials[4 * segment : 4 * segment + 4]
        for first, second in couples:
            other = baseline if second is None else portion[second]
            rows.append(jnp.sum(weights * portion[first] * other, axis=-1))
    return jnp.stack(rows)


def on_knots(rows, knot_hits, span):
    placed = jnp.dot(rows, knot_hits, precision=lax.Precision.HIGHEST)
    count = rows.shape[0] // 4
    total = jnp.zeros((count, span + 3), jnp.float32)
    for segment in range(4):
        part = placed[count * segment : count * (segment + 1)]
        total = total + jnp.pad(part, ((0, 0), (segment, 3 - segment)))
    return total


def body(
    residual,
    obs_weight,
    source_partials,
    attitude_partials,
    source_index,
    tile_pixel,
    tile_knot,
    pixel_slot,
):
    owners = lax.axis_size("sky")
    times = lax.axis_size("tm")
    chunks = owners * times
    run = PIX_DEV // times
    span = KNOTS_DEV // owners
    block = lax.axis_index("tm") * owners + lax.axis_index("sky")

    sums = local_sums(
        tile_pixel, pixel_slot, residual, obs_weight, source_partials, source_index, chunks
    )
    summed = reduce_chunks(sums)

    knot_start = tile_knot - block * span
    knot_hits = (knot_start[:, None] == jnp.arange(span, dtype=jnp.int32)[None, :]).astype(
        jnp.float32
    )
    square_rows = tile_rows(obs_weight, attitude_partials, None, KNOT_PAIRS)
    squares = on_knots(square_rows, knot_hits, span)

    update = damped_solve(summed[:15], summed[15:], 5, SOURCE_PAIRS)
    table = lax.all_gather(update, ("sky", "tm"), axis=0, tiled=False)
    settled = settle(
        tile_pixel,
        pixel_slot,
        residual,
        source_partials,
        source_index,
        table.reshape(chunks * 5 * run, SRC_PIX),
        run,
    )
    mine = lax.dynamic_slice_in_dim(table, lax.axis_index("sky") * times, times, 0)
    source_update = mine.transpose(1, 0, 2, 3).reshape(5, PIX_DEV * SRC_PIX)

    target_rows = tile_rows(
        obs_weight, attitude_partials, settled, [(first, None) for first in range(4)]
    )
    targets = on_knots(target_rows, knot_hits, span)
    accumulated = jnp.concatenate([squares, targets], axis=0)
    axes = ("tm", "sky")
    arriving = passed_along(accumulated[:, span:], axes, 1)
    whole = accumulated[:, :span] + jnp.pad(arriving, ((0, 0), (0, span - 3)))
    own_update = damped_solve(whole[:10], whole[10:], 4, KNOT_PAIRS)
    following = passed_along(own_update[:, :3], axes, -1)
    extended = jnp.concatenate([own_update, following], axis=1)
    attitude_update = lax.all_gather(own_update, "sky", axis=1, tiled=True)
    windows = jnp.concatenate([extended[:, seg : seg + span] for seg in range(4)], axis=0)
    values = jnp.dot(windows, knot_hits.T, precision=lax.Precision.HIGHEST)
    total = None
    for number in range(16):
        addend = attitude_partials[number] * values[number][:, None]
        total = addend if total is None else total + addend
    return (settled - total, source_update, attitude_update)


def reduce_chunks(sums):
    part = lax.psum_scatter(sums, ("sky", "tm"), scatter_dimension=0, tiled=True)
    return part[0]


def solution(mesh):
    in_specs = (
        P(("tm", "sky"), None),
        P(("tm", "sky"), None),
        P(None, ("tm", "sky"), None),
        P(None, ("tm", "sky"), None),
        P(("tm", "sky"), None),
        P(("tm", "sky")),
        P(("tm", "sky")),
        P(),
    )
    out_specs = (P(("tm", "sky"), None), P(None, "sky"), P(None, "tm"))
    return jax.shard_map(body, mesh=mesh, in_specs=in_specs, out_specs=out_specs, check_vma=False)
```

```python
import functools

import jax
import jax.numpy as jnp
from jax import lax
from jax.experimental import pallas as pl
from jax.experimental.pallas import tpu as pltpu
from jax.sharding import PartitionSpec as P

PIX_DEV = 128
SRC_PIX = 128
KNOTS_DEV = 512


SOURCE_PAIRS = tuple(((first, second) for first in range(5) for second in range(first, 5)))
KNOT_PAIRS = tuple(((first, second) for first in range(4) for second in range(first, 4)))


def passed_along(value, axes, steps):
    count = 1
    for axis in axes:
        count *= lax.axis_size(axis)
    first, last = (max(0, -steps), min(count, count - steps))
    return lax.ppermute(value, axes, [(source, source + steps) for source in range(first, last)])


def damped_solve(normal, target, order, pairs):
    entries = {}
    for number, couple in enumerate(pairs):
        entries[couple] = normal[number]
    factor = {}
    for column in range(order):
        pivot_value = entries[column, column] + 1.0
        for earlier in range(column):
            pivot_value = pivot_value - factor[column, earlier] * factor[column, earlier]
        pivot_value = jnp.sqrt(pivot_value)
        factor[column, column] = pivot_value
        for below in range(column + 1, order):
            current = entries[column, below]
            for earlier in range(column):
                current = current - factor[below, earlier] * factor[column, earlier]
            factor[below, column] = current / pivot_value
    forward = []
    for column in range(order):
        current = target[column]
        for earlier in range(column):
            current = current - factor[column, earlier] * forward[earlier]
        forward.append(current / factor[column, column])
    answer = [None] * order
    for column in reversed(range(order)):
        current = forward[column]
        for later in range(column + 1, order):
            current = current - factor[later, column] * answer[later]
        answer[column] = current / factor[column, column]
    return jnp.stack(answer)


ROWS = 20
PAD = 24


def sums_kernel(pixel_ref, slot_ref, resid, weight, parts, index, out, acc, stage):
    tiles = resid.shape[0]
    chunks, _, run, _ = out.shape
    pixels = chunks * run

    def clear(step, carry):
        acc[pl.ds(pl.multiple_of(step * 192, 192), 192), :] = jnp.zeros((192, SRC_PIX), jnp.float32)
        return carry

    lax.fori_loop(0, pixels * PAD // 192, clear, 0)
    stage[...] = jnp.zeros_like(stage)
    sources = lax.broadcasted_iota(jnp.int32, (SRC_PIX, SRC_PIX), 0)

    def group(step, carry):
        base = pl.multiple_of(step * 8, 8)
        here = pl.ds(base, 8)
        fields = [parts[c, here, :] for c in range(5)]
        scaled = [weight[here, :] * field for field in fields]
        baseline = resid[here, :]
        row = 0
        for first, second in SOURCE_PAIRS:
            stage[pl.ds(row, 8, stride=PAD), :] = scaled[first] * fields[second]
            row += 1
        for first in range(5):
            stage[pl.ds(row, 8, stride=PAD), :] = scaled[first] * baseline
            row += 1
        ids = index[here, :]
        for j in range(8):
            seat = slot_ref[pixel_ref[base + j]]
            values = stage[j * PAD : (j + 1) * PAD, :]
            high = values.astype(jnp.bfloat16)
            low = (values - high.astype(jnp.float32)).astype(jnp.bfloat16)
            hits = jnp.where(sources == ids[j : j + 1, :], 1.0, 0.0).astype(jnp.bfloat16)
            both = lax.dot_general(
                jnp.concatenate([high, low], axis=0),
                hits,
                (((1,), (1,)), ((), ())),
                preferred_element_type=jnp.float32,
            )
            spot = pl.ds(pl.multiple_of(seat * PAD, 8), PAD)
            acc[spot, :] += both[:PAD] + both[PAD:]
        return carry

    lax.fori_loop(0, tiles // 8, group, 0)

    def unload(chunk, carry):
        for row in range(ROWS):
            for part in range(run // 8):
                start = (chunk * run + part * 8) * PAD + row
                out[chunk, row, part * 8 : part * 8 + 8, :] = acc[pl.ds(start, 8, stride=PAD), :]
        return carry

    lax.fori_loop(0, chunks, unload, 0)


def local_sums(tile_pixel, pixel_slot, residual, obs_weight, source_partials, source_index, chunks):
    pixels = pixel_slot.shape[0]
    return pl.pallas_call(
        sums_kernel,
        name="local_sums",
        out_shape=jax.ShapeDtypeStruct((chunks, ROWS, pixels // chunks, SRC_PIX), jnp.float32),
        in_specs=[pl.BlockSpec(memory_space=pltpu.SMEM)] * 2
        + [pl.BlockSpec(memory_space=pltpu.VMEM)] * 4,
        out_specs=pl.BlockSpec(memory_space=pltpu.VMEM),
        scratch_shapes=[
            pltpu.VMEM((pixels * PAD, SRC_PIX), jnp.float32),
            pltpu.VMEM((8 * PAD, SRC_PIX), jnp.float32),
        ],
        compiler_params=pltpu.CompilerParams(vmem_limit_bytes=60 * 1024 * 1024),
    )(tile_pixel, pixel_slot, residual, obs_weight, source_partials, source_index)


def settle_kernel(run, pixel_ref, slot_ref, resid, parts, index, table, out, rows):
    tiles = resid.shape[0]

    def group(step, carry):
        base = pl.multiple_of(step * 8, 8)
        here = pl.ds(base, 8)
        for j in range(8):
            seat = slot_ref[pixel_ref[base + j]]
            start = (seat // run) * (5 * run) + seat % run
            for c in range(5):
                rows[c, pl.ds(base + j, 1), :] = table[pl.ds(start + c * run, 1), :]
        ids = index[here, :]
        total = None
        for c in range(5):
            picked = jnp.take_along_axis(rows[c, here, :], ids, axis=1)
            addend = parts[c, here, :] * picked
            total = addend if total is None else total + addend
        out[here, :] = resid[here, :] - total
        return carry

    lax.fori_loop(0, tiles // 8, group, 0)


def settle(tile_pixel, pixel_slot, residual, source_partials, source_index, table, run):
    tiles = residual.shape[0]
    return pl.pallas_call(
        functools.partial(settle_kernel, run),
        name="settle",
        out_shape=jax.ShapeDtypeStruct(residual.shape, jnp.float32),
        in_specs=[pl.BlockSpec(memory_space=pltpu.SMEM)] * 2
        + [pl.BlockSpec(memory_space=pltpu.VMEM)] * 4,
        out_specs=pl.BlockSpec(memory_space=pltpu.VMEM),
        scratch_shapes=[pltpu.VMEM((5, tiles, SRC_PIX), jnp.float32)],
        compiler_params=pltpu.CompilerParams(vmem_limit_bytes=48 * 1024 * 1024),
    )(tile_pixel, pixel_slot, residual, source_partials, source_index, table)


def tile_rows(weights, partials, baseline, couples):
    rows = []
    for segment in range(4):
        portion = partials[4 * segment : 4 * segment + 4]
        for first, second in couples:
            other = baseline if second is None else portion[second]
            rows.append(jnp.sum(weights * portion[first] * other, axis=-1))
    return jnp.stack(rows)


def on_knots(rows, knot_hits, span):
    placed = jnp.dot(rows, knot_hits, precision=lax.Precision.HIGHEST)
    count = rows.shape[0] // 4
    total = jnp.zeros((count, span + 3), jnp.float32)
    for segment in range(4):
        part = placed[count * segment : count * (segment + 1)]
        total = total + jnp.pad(part, ((0, 0), (segment, 3 - segment)))
    return total


def body(
    residual,
    obs_weight,
    source_partials,
    attitude_partials,
    source_index,
    tile_pixel,
    tile_knot,
    pixel_slot,
):
    owners = lax.axis_size("sky")
    times = lax.axis_size("tm")
    chunks = owners * times
    run = PIX_DEV // times
    span = KNOTS_DEV // owners
    block = lax.axis_index("tm") * owners + lax.axis_index("sky")

    sums = local_sums(
        tile_pixel, pixel_slot, residual, obs_weight, source_partials, source_index, chunks
    )
    summed, late_weight = lax.optimization_barrier((reduce_chunks(sums), obs_weight))

    knot_start = tile_knot - block * span
    knot_hits = (knot_start[:, None] == jnp.arange(span, dtype=jnp.int32)[None, :]).astype(
        jnp.float32
    )
    square_rows = tile_rows(late_weight, attitude_partials, None, KNOT_PAIRS)
    squares = on_knots(square_rows, knot_hits, span)

    update = damped_solve(summed[:15], summed[15:], 5, SOURCE_PAIRS)
    table = lax.all_gather(update, ("sky", "tm"), axis=0, tiled=False)
    settled = settle(
        tile_pixel,
        pixel_slot,
        residual,
        source_partials,
        source_index,
        table.reshape(chunks * 5 * run, SRC_PIX),
        run,
    )
    mine = lax.dynamic_slice_in_dim(table, lax.axis_index("sky") * times, times, 0)
    source_update = mine.transpose(1, 0, 2, 3).reshape(5, PIX_DEV * SRC_PIX)

    target_rows = tile_rows(
        obs_weight, attitude_partials, settled, [(first, None) for first in range(4)]
    )
    targets = on_knots(target_rows, knot_hits, span)
    accumulated = jnp.concatenate([squares, targets], axis=0)
    axes = ("tm", "sky")
    arriving = passed_along(accumulated[:, span:], axes, 1)
    whole = accumulated[:, :span] + jnp.pad(arriving, ((0, 0), (0, span - 3)))
    own_update = damped_solve(whole[:10], whole[10:], 4, KNOT_PAIRS)
    following = passed_along(own_update[:, :3], axes, -1)
    extended = jnp.concatenate([own_update, following], axis=1)
    attitude_update = lax.all_gather(own_update, "sky", axis=1, tiled=True)
    windows = jnp.concatenate([extended[:, seg : seg + span] for seg in range(4)], axis=0)
    values = jnp.dot(windows, knot_hits.T, precision=lax.Precision.HIGHEST)
    total = None
    for number in range(16):
        addend = attitude_partials[number] * values[number][:, None]
        total = addend if total is None else total + addend
    return (settled - total, source_update, attitude_update)


def add_rows(count, target, *sources):
    def one(row, carry):
        total = sources[0][row]
        for source in sources[1:]:
            total = total + source[row]
        target[row] = total
        return carry

    lax.fori_loop(0, count, one, 0)


def reduce_kernel(times, lines, sums, out, got0, got1, part, got2, *sems):
    send0, recv0, send1, recv1, send2, recv2 = sems
    mesh_ids = pl.DeviceIdType.MESH
    time, sky = lax.axis_index("tm"), lax.axis_index("sky")
    line, core = sky // 2, sky % 2
    time_peers = [lax.rem(time + step, times) for step in range(1, times)]
    line_peers = [lax.rem(line + step, lines) for step in range(1, lines)]
    partner = (time, sky + 1 - 2 * core)

    barrier = pltpu.get_barrier_semaphore()
    peers = [partner] + [(peer, sky) for peer in time_peers]
    peers += [(time, peer * 2 + core) for peer in line_peers]
    for peer in peers:
        pl.semaphore_signal(barrier, inc=1, device_id=peer, device_id_type=mesh_ids)
    pl.semaphore_wait(barrier, len(peers))

    pieces = line_peers + [line]
    first = []
    for step, piece in enumerate(pieces):
        copy = pltpu.make_async_remote_copy(
            src_ref=sums.at[piece, 1 - core],
            dst_ref=got0.at[step],
            send_sem=send0.at[step],
            recv_sem=recv0.at[step],
            device_id=partner,
            device_id_type=mesh_ids,
        )
        copy.start()
        first.append(copy)
    second = []
    for step, piece in enumerate(pieces):
        first[step].wait_recv()
        for slot in range(times):
            target = got0.at[step, slot]
            add_rows(ROWS, target, target, sums.at[piece, core, slot])
        copies = []
        for number, peer in enumerate(time_peers):
            copy = pltpu.make_async_remote_copy(
                src_ref=got0.at[step, peer],
                dst_ref=got1.at[step, number],
                send_sem=send1.at[step, number],
                recv_sem=recv1.at[step, number],
                device_id=(peer, sky),
                device_id_type=mesh_ids,
            )
            copy.start()
            copies.append(copy)
        second.append(copies)
    third = []
    for step, piece in enumerate(pieces):
        for copy in second[step]:
            copy.wait_recv()
        arrived = [got1.at[step, number] for number in range(times - 1)]
        add_rows(ROWS, part.at[step], got0.at[step, time], *arrived)
        if step < lines - 1:
            copy = pltpu.make_async_remote_copy(
                src_ref=part.at[step],
                dst_ref=got2.at[step],
                send_sem=send2.at[step],
                recv_sem=recv2.at[step],
                device_id=(time, piece * 2 + core),
                device_id_type=mesh_ids,
            )
            copy.start()
            third.append(copy)
    for copy in third:
        copy.wait_recv()
    arrived = [got2.at[step] for step in range(lines - 1)]
    add_rows(ROWS, out, part.at[lines - 1], *arrived)
    for copy in first + [copy for copies in second for copy in copies] + third:
        copy.wait_send()


def reduce_chunks(sums):
    times, owners = lax.axis_size("tm"), lax.axis_size("sky")
    lines = owners // 2
    unit = sums.shape[1:]
    dma = pltpu.SemaphoreType.DMA
    return pl.pallas_call(
        functools.partial(reduce_kernel, times, lines),
        name="reduce_chunks",
        out_shape=jax.ShapeDtypeStruct(unit, jnp.float32),
        in_specs=[pl.BlockSpec(memory_space=pltpu.VMEM)],
        out_specs=pl.BlockSpec(memory_space=pltpu.VMEM),
        scratch_shapes=[
            pltpu.VMEM((lines, times) + unit, jnp.float32),
            pltpu.VMEM((lines, times - 1) + unit, jnp.float32),
            pltpu.VMEM((lines,) + unit, jnp.float32),
            pltpu.VMEM((lines - 1,) + unit, jnp.float32),
            dma((lines,)),
            dma((lines,)),
            dma((lines, times - 1)),
            dma((lines, times - 1)),
            dma((lines - 1,)),
            dma((lines - 1,)),
        ],
        compiler_params=pltpu.CompilerParams(
            collective_id=0, has_side_effects=True, vmem_limit_bytes=62 * 1024 * 1024
        ),
    )(sums.reshape((lines, 2, times) + unit))


def solution(mesh):
    in_specs = (
        P(("tm", "sky"), None),
        P(("tm", "sky"), None),
        P(None, ("tm", "sky"), None),
        P(None, ("tm", "sky"), None),
        P(("tm", "sky"), None),
        P(("tm", "sky")),
        P(("tm", "sky")),
        P(),
    )
    out_specs = (P(("tm", "sky"), None), P(None, "sky"), P(None, "tm"))
    return jax.shard_map(body, mesh=mesh, in_specs=in_specs, out_specs=out_specs, check_vma=False)
```

```python
import functools

import jax
import jax.numpy as jnp
from jax import lax
from jax.experimental import pallas as pl
from jax.experimental.pallas import tpu as pltpu
from jax.sharding import PartitionSpec as P

PIX_DEV = 128
SRC_PIX = 128
KNOTS_DEV = 512


SOURCE_PAIRS = tuple(((first, second) for first in range(5) for second in range(first, 5)))
KNOT_PAIRS = tuple(((first, second) for first in range(4) for second in range(first, 4)))


def passed_along(value, axes, steps):
    count = 1
    for axis in axes:
        count *= lax.axis_size(axis)
    first, last = (max(0, -steps), min(count, count - steps))
    return lax.ppermute(value, axes, [(source, source + steps) for source in range(first, last)])


def damped_solve(normal, target, order, pairs):
    entries = {}
    for number, couple in enumerate(pairs):
        entries[couple] = normal[number]
    factor = {}
    for column in range(order):
        pivot_value = entries[column, column] + 1.0
        for earlier in range(column):
            pivot_value = pivot_value - factor[column, earlier] * factor[column, earlier]
        pivot_value = jnp.sqrt(pivot_value)
        factor[column, column] = pivot_value
        for below in range(column + 1, order):
            current = entries[column, below]
            for earlier in range(column):
                current = current - factor[below, earlier] * factor[column, earlier]
            factor[below, column] = current / pivot_value
    forward = []
    for column in range(order):
        current = target[column]
        for earlier in range(column):
            current = current - factor[column, earlier] * forward[earlier]
        forward.append(current / factor[column, column])
    answer = [None] * order
    for column in reversed(range(order)):
        current = forward[column]
        for later in range(column + 1, order):
            current = current - factor[later, column] * answer[later]
        answer[column] = current / factor[column, column]
    return jnp.stack(answer)


ROWS = 20
PAD = 24


def sums_kernel(pixel_ref, slot_ref, resid, weight, parts, index, out, acc, stage):
    tiles = resid.shape[0]
    chunks, _, run, _ = out.shape
    pixels = chunks * run

    def clear(step, carry):
        acc[pl.ds(pl.multiple_of(step * 192, 192), 192), :] = jnp.zeros((192, SRC_PIX), jnp.float32)
        return carry

    lax.fori_loop(0, pixels * PAD // 192, clear, 0)
    stage[...] = jnp.zeros_like(stage)
    sources = lax.broadcasted_iota(jnp.int32, (SRC_PIX, SRC_PIX), 0)

    def group(step, carry):
        base = pl.multiple_of(step * 8, 8)
        here = pl.ds(base, 8)
        fields = [parts[c, here, :] for c in range(5)]
        scaled = [weight[here, :] * field for field in fields]
        baseline = resid[here, :]
        row = 0
        for first, second in SOURCE_PAIRS:
            stage[pl.ds(row, 8, stride=PAD), :] = scaled[first] * fields[second]
            row += 1
        for first in range(5):
            stage[pl.ds(row, 8, stride=PAD), :] = scaled[first] * baseline
            row += 1
        ids = index[here, :]
        for j in range(8):
            seat = slot_ref[pixel_ref[base + j]]
            values = stage[j * PAD : (j + 1) * PAD, :]
            high = values.astype(jnp.bfloat16)
            low = (values - high.astype(jnp.float32)).astype(jnp.bfloat16)
            hits = jnp.where(sources == ids[j : j + 1, :], 1.0, 0.0).astype(jnp.bfloat16)
            both = lax.dot_general(
                jnp.concatenate([high, low], axis=0),
                hits,
                (((1,), (1,)), ((), ())),
                preferred_element_type=jnp.float32,
            )
            spot = pl.ds(pl.multiple_of(seat * PAD, 8), PAD)
            acc[spot, :] += both[:PAD] + both[PAD:]
        return carry

    lax.fori_loop(0, tiles // 8, group, 0)

    def unload(chunk, carry):
        for row in range(ROWS):
            for part in range(run // 8):
                start = (chunk * run + part * 8) * PAD + row
                out[chunk, row, part * 8 : part * 8 + 8, :] = acc[pl.ds(start, 8, stride=PAD), :]
        return carry

    lax.fori_loop(0, chunks, unload, 0)


def local_sums(tile_pixel, pixel_slot, residual, obs_weight, source_partials, source_index, chunks):
    pixels = pixel_slot.shape[0]
    return pl.pallas_call(
        sums_kernel,
        name="local_sums",
        out_shape=jax.ShapeDtypeStruct((chunks, ROWS, pixels // chunks, SRC_PIX), jnp.float32),
        in_specs=[pl.BlockSpec(memory_space=pltpu.SMEM)] * 2
        + [pl.BlockSpec(memory_space=pltpu.VMEM)] * 4,
        out_specs=pl.BlockSpec(memory_space=pltpu.VMEM),
        scratch_shapes=[
            pltpu.VMEM((pixels * PAD, SRC_PIX), jnp.float32),
            pltpu.VMEM((8 * PAD, SRC_PIX), jnp.float32),
        ],
        compiler_params=pltpu.CompilerParams(vmem_limit_bytes=60 * 1024 * 1024),
    )(tile_pixel, pixel_slot, residual, obs_weight, source_partials, source_index)


def settle_kernel(run, pixel_ref, slot_ref, resid, parts, index, table, out, rows):
    tiles = resid.shape[0]

    def group(step, carry):
        base = pl.multiple_of(step * 8, 8)
        here = pl.ds(base, 8)
        for j in range(8):
            seat = slot_ref[pixel_ref[base + j]]
            start = (seat // run) * (5 * run) + seat % run
            for c in range(5):
                rows[c, pl.ds(base + j, 1), :] = table[pl.ds(start + c * run, 1), :]
        ids = index[here, :]
        total = None
        for c in range(5):
            picked = jnp.take_along_axis(rows[c, here, :], ids, axis=1)
            addend = parts[c, here, :] * picked
            total = addend if total is None else total + addend
        out[here, :] = resid[here, :] - total
        return carry

    lax.fori_loop(0, tiles // 8, group, 0)


def settle(tile_pixel, pixel_slot, residual, source_partials, source_index, table, run):
    tiles = residual.shape[0]
    return pl.pallas_call(
        functools.partial(settle_kernel, run),
        name="settle",
        out_shape=jax.ShapeDtypeStruct(residual.shape, jnp.float32),
        in_specs=[pl.BlockSpec(memory_space=pltpu.SMEM)] * 2
        + [pl.BlockSpec(memory_space=pltpu.VMEM)] * 4,
        out_specs=pl.BlockSpec(memory_space=pltpu.VMEM),
        scratch_shapes=[pltpu.VMEM((5, tiles, SRC_PIX), jnp.float32)],
        compiler_params=pltpu.CompilerParams(vmem_limit_bytes=48 * 1024 * 1024),
    )(tile_pixel, pixel_slot, residual, source_partials, source_index, table)


def tile_rows(weights, partials, baseline, couples):
    rows = []
    for segment in range(4):
        portion = partials[4 * segment : 4 * segment + 4]
        for first, second in couples:
            other = baseline if second is None else portion[second]
            rows.append(jnp.sum(weights * portion[first] * other, axis=-1))
    return jnp.stack(rows)


def on_knots(rows, knot_hits, span):
    placed = jnp.dot(rows, knot_hits, precision=lax.Precision.HIGHEST)
    count = rows.shape[0] // 4
    total = jnp.zeros((count, span + 3), jnp.float32)
    for segment in range(4):
        part = placed[count * segment : count * (segment + 1)]
        total = total + jnp.pad(part, ((0, 0), (segment, 3 - segment)))
    return total


def body(
    residual,
    obs_weight,
    source_partials,
    attitude_partials,
    source_index,
    tile_pixel,
    tile_knot,
    pixel_slot,
):
    owners = lax.axis_size("sky")
    times = lax.axis_size("tm")
    chunks = owners * times
    run = PIX_DEV // times
    span = KNOTS_DEV // owners
    block = lax.axis_index("tm") * owners + lax.axis_index("sky")

    sums = local_sums(
        tile_pixel, pixel_slot, residual, obs_weight, source_partials, source_index, chunks
    )
    summed, late_weight = lax.optimization_barrier((reduce_chunks(sums), obs_weight))

    knot_start = tile_knot - block * span
    knot_hits = (knot_start[:, None] == jnp.arange(span, dtype=jnp.int32)[None, :]).astype(
        jnp.float32
    )
    square_rows = tile_rows(late_weight, attitude_partials, None, KNOT_PAIRS)
    squares = on_knots(square_rows, knot_hits, span)

    update = damped_solve(summed[:15], summed[15:], 5, SOURCE_PAIRS)
    table = gather_chunks(update)
    settled = settle(
        tile_pixel,
        pixel_slot,
        residual,
        source_partials,
        source_index,
        table.reshape(chunks * 5 * run, SRC_PIX),
        run,
    )
    mine = lax.dynamic_slice_in_dim(table, lax.axis_index("sky") * times, times, 0)
    source_update = mine.transpose(1, 0, 2, 3).reshape(5, PIX_DEV * SRC_PIX)

    target_rows = tile_rows(
        obs_weight, attitude_partials, settled, [(first, None) for first in range(4)]
    )
    targets = on_knots(target_rows, knot_hits, span)
    accumulated = jnp.concatenate([squares, targets], axis=0)
    axes = ("tm", "sky")
    arriving = passed_along(accumulated[:, span:], axes, 1)
    whole = accumulated[:, :span] + jnp.pad(arriving, ((0, 0), (0, span - 3)))
    own_update = damped_solve(whole[:10], whole[10:], 4, KNOT_PAIRS)
    following = passed_along(own_update[:, :3], axes, -1)
    extended = jnp.concatenate([own_update, following], axis=1)
    attitude_update = lax.all_gather(own_update, "sky", axis=1, tiled=True)
    windows = jnp.concatenate([extended[:, seg : seg + span] for seg in range(4)], axis=0)
    values = jnp.dot(windows, knot_hits.T, precision=lax.Precision.HIGHEST)
    total = None
    for number in range(16):
        addend = attitude_partials[number] * values[number][:, None]
        total = addend if total is None else total + addend
    return (settled - total, source_update, attitude_update)


def add_rows(count, target, *sources):
    def one(row, carry):
        total = sources[0][row]
        for source in sources[1:]:
            total = total + source[row]
        target[row] = total
        return carry

    lax.fori_loop(0, count, one, 0)


def reduce_kernel(times, lines, sums, out, got0, got1, part, got2, *sems):
    send0, recv0, send1, recv1, send2, recv2 = sems
    mesh_ids = pl.DeviceIdType.MESH
    time, sky = lax.axis_index("tm"), lax.axis_index("sky")
    line, core = sky // 2, sky % 2
    time_peers = [lax.rem(time + step, times) for step in range(1, times)]
    line_peers = [lax.rem(line + step, lines) for step in range(1, lines)]
    partner = (time, sky + 1 - 2 * core)

    barrier = pltpu.get_barrier_semaphore()
    peers = [partner] + [(peer, sky) for peer in time_peers]
    peers += [(time, peer * 2 + core) for peer in line_peers]
    for peer in peers:
        pl.semaphore_signal(barrier, inc=1, device_id=peer, device_id_type=mesh_ids)
    pl.semaphore_wait(barrier, len(peers))

    pieces = line_peers + [line]
    first = []
    for step, piece in enumerate(pieces):
        copy = pltpu.make_async_remote_copy(
            src_ref=sums.at[piece, 1 - core],
            dst_ref=got0.at[step],
            send_sem=send0.at[step],
            recv_sem=recv0.at[step],
            device_id=partner,
            device_id_type=mesh_ids,
        )
        copy.start()
        first.append(copy)
    second = []
    for step, piece in enumerate(pieces):
        first[step].wait_recv()
        for slot in range(times):
            target = got0.at[step, slot]
            add_rows(ROWS, target, target, sums.at[piece, core, slot])
        copies = []
        for number, peer in enumerate(time_peers):
            copy = pltpu.make_async_remote_copy(
                src_ref=got0.at[step, peer],
                dst_ref=got1.at[step, number],
                send_sem=send1.at[step, number],
                recv_sem=recv1.at[step, number],
                device_id=(peer, sky),
                device_id_type=mesh_ids,
            )
            copy.start()
            copies.append(copy)
        second.append(copies)
    third = []
    for step, piece in enumerate(pieces):
        for copy in second[step]:
            copy.wait_recv()
        arrived = [got1.at[step, number] for number in range(times - 1)]
        add_rows(ROWS, part.at[step], got0.at[step, time], *arrived)
        if step < lines - 1:
            copy = pltpu.make_async_remote_copy(
                src_ref=part.at[step],
                dst_ref=got2.at[step],
                send_sem=send2.at[step],
                recv_sem=recv2.at[step],
                device_id=(time, piece * 2 + core),
                device_id_type=mesh_ids,
            )
            copy.start()
            third.append(copy)
    for copy in third:
        copy.wait_recv()
    arrived = [got2.at[step] for step in range(lines - 1)]
    add_rows(ROWS, out, part.at[lines - 1], *arrived)
    for copy in first + [copy for copies in second for copy in copies] + third:
        copy.wait_send()


def reduce_chunks(sums):
    times, owners = lax.axis_size("tm"), lax.axis_size("sky")
    lines = owners // 2
    unit = sums.shape[1:]
    dma = pltpu.SemaphoreType.DMA
    return pl.pallas_call(
        functools.partial(reduce_kernel, times, lines),
        name="reduce_chunks",
        out_shape=jax.ShapeDtypeStruct(unit, jnp.float32),
        in_specs=[pl.BlockSpec(memory_space=pltpu.VMEM)],
        out_specs=pl.BlockSpec(memory_space=pltpu.VMEM),
        scratch_shapes=[
            pltpu.VMEM((lines, times) + unit, jnp.float32),
            pltpu.VMEM((lines, times - 1) + unit, jnp.float32),
            pltpu.VMEM((lines,) + unit, jnp.float32),
            pltpu.VMEM((lines - 1,) + unit, jnp.float32),
            dma((lines,)),
            dma((lines,)),
            dma((lines, times - 1)),
            dma((lines, times - 1)),
            dma((lines - 1,)),
            dma((lines - 1,)),
        ],
        compiler_params=pltpu.CompilerParams(
            collective_id=0, has_side_effects=True, vmem_limit_bytes=62 * 1024 * 1024
        ),
    )(sums.reshape((lines, 2, times) + unit))


def gather_kernel(times, lines, update, table, send0, recv0, send1, recv1, send2, recv2):
    mesh_ids = pl.DeviceIdType.MESH
    time, sky = lax.axis_index("tm"), lax.axis_index("sky")
    line, core = sky // 2, sky % 2
    time_peers = [lax.rem(time + step, times) for step in range(1, times)]
    line_peers = [lax.rem(line + step, lines) for step in range(1, lines)]
    partner = (time, sky + 1 - 2 * core)

    barrier = pltpu.get_barrier_semaphore()
    peers = [partner] + [(peer, sky) for peer in time_peers]
    peers += [(time, peer * 2 + core) for peer in line_peers]
    for peer in peers:
        pl.semaphore_signal(barrier, inc=1, device_id=peer, device_id_type=mesh_ids)
    pl.semaphore_wait(barrier, len(peers))

    def send(source, target, send_sem, recv_sem, peer):
        copy = pltpu.make_async_remote_copy(
            src_ref=source,
            dst_ref=target,
            send_sem=send_sem,
            recv_sem=recv_sem,
            device_id=peer,
            device_id_type=mesh_ids,
        )
        copy.start()
        return copy

    own = table.at[sky * times + time]
    first = []
    for number, peer in enumerate(line_peers):
        spot = (time, peer * 2 + core)
        first.append(send(update, own, send0.at[number], recv0.at[number], spot))
    own[...] = update[...]
    sources = [line] + [lax.rem(line + lines - step, lines) for step in range(1, lines)]
    second = []
    for step, source in enumerate(sources):
        place = table.at[(source * 2 + core) * times + time]
        if step > 0:
            first[step - 1].wait_recv()
        held = place if step > 0 else update
        second.append(
            [
                send(held, place, send1.at[step, number], recv1.at[step, number], (peer, sky))
                for number, peer in enumerate(time_peers)
            ]
        )
    third = []
    for step, source in enumerate(sources):
        for copy in second[step]:
            copy.wait_recv()
        place = table.at[pl.ds((source * 2 + core) * times, times)]
        third.append(send(place, place, send2.at[step], recv2.at[step], partner))
    for copy in third:
        copy.wait_recv()
    for copy in first + [copy for copies in second for copy in copies] + third:
        copy.wait_send()


def gather_chunks(update):
    times, owners = lax.axis_size("tm"), lax.axis_size("sky")
    lines = owners // 2
    dma = pltpu.SemaphoreType.DMA
    return pl.pallas_call(
        functools.partial(gather_kernel, times, lines),
        name="gather_chunks",
        out_shape=jax.ShapeDtypeStruct((owners * times,) + update.shape, jnp.float32),
        in_specs=[pl.BlockSpec(memory_space=pltpu.VMEM)],
        out_specs=pl.BlockSpec(memory_space=pltpu.VMEM),
        scratch_shapes=[
            dma((lines - 1,)),
            dma((lines - 1,)),
            dma((lines, times - 1)),
            dma((lines, times - 1)),
            dma((lines,)),
            dma((lines,)),
        ],
        compiler_params=pltpu.CompilerParams(
            collective_id=1, has_side_effects=True, vmem_limit_bytes=16 * 1024 * 1024
        ),
    )(update)


def solution(mesh):
    in_specs = (
        P(("tm", "sky"), None),
        P(("tm", "sky"), None),
        P(None, ("tm", "sky"), None),
        P(None, ("tm", "sky"), None),
        P(("tm", "sky"), None),
        P(("tm", "sky")),
        P(("tm", "sky")),
        P(),
    )
    out_specs = (P(("tm", "sky"), None), P(None, "sky"), P(None, "tm"))
    return jax.shard_map(body, mesh=mesh, in_specs=in_specs, out_specs=out_specs, check_vma=False)
```
